32 devices in a mesh: lat: 8 (over y, x, core), lev: 4 (over z).
Axes of the slice: x: 2, y: 2, z: 4, core: 2. Of those that a mesh axis runs over, the one named last changes fastest.
Arguments:
- fields: float32 [12, 128, 256, 1024], P(None, 'lev', 'lat'), may hold values from -6 to 6
- legendre: bfloat16 [256, 256, 256], P('lat'), as said below
- owner_counts: int32 [8], replicated, may hold values from 1 to 64, 256 in all
Outputs:
- covariance: float32 [512, 128, 128], P('lat', 'lev')
The draws below stay inside these ranges and needn't reach their ends.
Inputs may be any that keep to these rules, and one draw needn't show every extreme that they name: `owner_counts`: each owner holds 1 to 64 total wavenumbers, the counts sum to 256, and some owner holds exactly 64. legendre[lat, m, n] is zero where n < m.
All inputs are finite; a program needn't handle non-finite values.
Results may differ from the reference program's by a relative error of at most 0.0038.
Values may be sent and summed in bfloat16 or wider, within the bound.
A program may use at most 192 MiB of HBM per device.

```python
import math
import jax
import jax.numpy as jnp
import numpy as np
from jax import lax

NLON = 1024
NLAT = 256
MTRUNC = 256
LEV = 128
MEM = 12
NCAP = 64
OWNERS = 8


def draw_legendre(key, part):
    values = jax.random.normal(key, (NLAT, MTRUNC, MTRUNC), jnp.float32) * NLAT ** (-0.5)
    order = jnp.arange(MTRUNC, dtype=jnp.int32)
    keeper = order[None, :] >= order[:, None]
    return jnp.where(keeper[None, :, :], values, jnp.zeros_like(values)).astype(jnp.bfloat16)


def levels(key, extent, shards, smallest, top_value):
    level = 1.0
    for position, parts in shards:
        draws = jax.random.uniform(jax.random.fold_in(jax.random.fold_in(key, 6), position), (parts,), jnp.float32, smallest / len(shards), top_value / len(shards))
        level = level * jnp.repeat(jnp.exp(draws), extent[position] // parts).reshape((-1,) + (1,) * (len(extent) - 1 - position))
    return level


def split_up(number_of, total, reach, slope):
    portions = [(1 << 20) // math.isqrt(rank ** slope) + 1 for rank in range(2, number_of + 1)]
    rest, given = total - reach - (number_of - 1), [1] * (number_of - 1)
    while rest > 0:
        candidates = [i for i in range(number_of - 1) if given[i] < reach]
        mass, remaining = sum([portions[i] for i in candidates]), rest
        for i in candidates:
            addition = min(reach - given[i], max(1, remaining * portions[i] // mass), rest)
            given[i] = given[i] + addition
            rest = rest - addition
    return np.array([reach] + given)


def ragged_sizes(key, number_of, total, most, skew):
    if number_of == 2:
        one = jax.random.randint(key, (), max(1, total - most), min(most, total - 1) + 1)
        return jnp.stack([one, total - one])
    lengths = jnp.asarray(split_up(number_of, total, most, skew), jnp.int32)
    couples = (number_of - 1) // 2
    giver, taker = lengths[1:1 + 2 * couples:2], lengths[2:2 + 2 * couples:2]
    room = jnp.minimum(giver - 1, most - taker)
    moved = jax.random.randint(jax.random.fold_in(key, 1), (couples,), 0, 1 << 20) % (room + 1)
    lengths = lengths.at[1:1 + 2 * couples:2].set(giver - moved).at[2:2 + 2 * couples:2].set(taker + moved)
    return lengths[jax.random.permutation(jax.random.fold_in(key, 2), number_of)]


def normal_values(key, shape, scale, most, split=(), kind=jnp.bfloat16):
    factor_of = levels(key, shape, split, -0.22, 0.18) if split else 1.0
    entries = jax.random.normal(key, shape, jnp.float32) * scale * factor_of
    return jnp.minimum(jnp.maximum(entries, -most), most).astype(kind)


def setup_inputs(seed: int = 0) -> dict:
    splits = jax.random.split(jax.random.key(seed), 4)
    return {
        "fields": normal_values(splits[0], (MEM, LEV, NLAT, NLON), 1.0, 6.0, ((1, 4), (2, 8)), jnp.float32),
        "legendre": draw_legendre(jax.random.fold_in(splits[3], 71), 0),
        "owner_counts": ragged_sizes(splits[2], OWNERS, MTRUNC, NCAP, 2).astype(jnp.int32),
    }


def reference(fields, legendre, owner_counts):
    transform = jnp.fft.rfft(fields, axis=-1)[..., :MTRUNC] * (NLON ** -0.5)
    stacked = jnp.stack([jnp.real(transform), jnp.imag(transform)], axis=0).astype(jnp.float32)
    spectra = jnp.transpose(stacked, (3, 4, 0, 1, 2)).astype(jnp.bfloat16)
    block_size = 32

    def add_block(running, block_id):
        spec_block = lax.dynamic_slice_in_dim(spectra, block_id * block_size, block_size, 1).astype(jnp.float32)
        transform_table_block = lax.dynamic_slice_in_dim(legendre, block_id * block_size, block_size, 1).astype(jnp.float32)
        wavenumber_rows = jnp.einsum('lmqbe,lmn->nmqbe', spec_block, transform_table_block)
        anomaly = (wavenumber_rows - jnp.mean(wavenumber_rows, axis=3, keepdims=True)).astype(jnp.bfloat16)
        anomaly = lax.optimization_barrier(anomaly).astype(jnp.float32)
        return running + jnp.einsum('nmqbe,nmqbk->nek', anomaly, anomaly), None

    blocks_all = jnp.arange(MTRUNC // block_size, dtype=jnp.int32)
    start_sum = jnp.zeros((MTRUNC, LEV, LEV), jnp.float32)
    full, unused = lax.scan(add_block, start_sum, blocks_all)
    wavenumber = jnp.arange(MTRUNC, dtype=jnp.int32)
    divisor = ((MEM - 1) * (2 * wavenumber + 2)).astype(jnp.float32)
    full = full / divisor[:, None, None]
    starts = (jnp.cumsum(owner_counts) - owner_counts).astype(jnp.int32)
    offset = jnp.arange(NCAP, dtype=jnp.int32)
    active_flag = offset[None, :] < owner_counts[:, None]
    slot_index = jnp.where(active_flag, starts[:, None] + offset[None, :], 0).reshape(-1).astype(jnp.int32)
    selected_entries = jnp.take(full, slot_index, axis=0)
    return jnp.where(active_flag.reshape(-1)[:, None, None], selected_entries, jnp.zeros_like(selected_entries))
```

```python
import functools
import math

import jax
import jax.numpy as jnp
import numpy as np
from jax import lax
from jax.experimental import pallas as pl
from jax.experimental.pallas import tpu as pltpu
from jax.sharding import PartitionSpec as P


def fourier_table(points, modes):
    places = jnp.arange(points, dtype=jnp.int32)
    orders = jnp.arange(modes, dtype=jnp.int32)
    phase = places[:, None] * orders[None, :] % points
    angle = phase.astype(jnp.float32) * (2.0 * math.pi / points)
    factor = points ** (-0.5)
    return jnp.stack([jnp.cos(angle) * factor, -jnp.sin(angle) * factor], axis=2)


def plain_on_device(fields, legendre, owner_counts):
    members, lev_rows, lat_rows, points = fields.shape
    modes = legendre.shape[1]
    lev_count = lax.axis_size("lev")
    owners = owner_counts.shape[0]
    capacity = 2 * modes // owners
    dft_table = fourier_table(points, modes)
    spectra = jnp.einsum("belx,xmc->lmcbe", fields, dft_table, precision=lax.Precision.HIGHEST)
    spectra = spectra.reshape(lat_rows, modes, 2 * members * lev_rows).astype(jnp.bfloat16)
    collected_rows, transform_table_rows = (
        lax.all_to_all(spectra, "lat", split_axis=1, concat_axis=0, tiled=True),
        lax.all_to_all(legendre, "lat", split_axis=1, concat_axis=0, tiled=True),
    )
    wavenumber_rows = jnp.einsum(
        "dez,det->tez", collected_rows, transform_table_rows, preferred_element_type=jnp.float32
    )
    resident_modes = wavenumber_rows.shape[1]
    shaped = wavenumber_rows.reshape(modes, resident_modes, 2, members, lev_rows)
    anomaly = (shaped - jnp.mean(shaped, axis=3, keepdims=True)).astype(jnp.bfloat16)
    anomaly = anomaly.reshape(modes, resident_modes, 2 * members * lev_rows)
    starts = jnp.cumsum(owner_counts) - owner_counts
    offset = jnp.arange(capacity, dtype=jnp.int32)
    active_flag = offset[None, :] < owner_counts[:, None]
    slot_index = jnp.where(active_flag, starts[:, None] + offset[None, :], 0).reshape(-1)
    slotted = jnp.take(anomaly, slot_index, axis=0)
    slotted = jnp.where(active_flag.reshape(-1)[:, None, None], slotted, jnp.zeros_like(slotted))
    slotted = slotted[None]
    received = lax.all_to_all(
        lax.all_to_all(slotted, "lat", split_axis=1, concat_axis=2, tiled=True),
        "lev",
        split_axis=2,
        concat_axis=0,
        tiled=True,
    )
    mode_share = received.shape[2]
    blocks = received.reshape(lev_count, capacity, mode_share, 2 * members, lev_rows)
    partial_value = jnp.einsum(
        "esaql,fsaqk->selfk", blocks, blocks, preferred_element_type=jnp.float32
    )
    partial_value = partial_value.reshape(capacity, lev_count * lev_rows, lev_count * lev_rows)
    summed = lax.psum_scatter(partial_value, "lev", scatter_dimension=1, tiled=True)
    owner = lax.axis_index("lat")
    wavenumber = starts[owner] + offset
    live_count = owner_counts[owner]
    divisor = ((members - 1) * (2 * wavenumber + 2)).astype(jnp.float32)
    scaled = summed / divisor[:, None, None]
    return jnp.where((offset < live_count)[:, None, None], scaled, jnp.zeros_like(scaled))


LANES = 128
VMEM_LIMIT = 60 * 1024 * 1024


def split_bf16(values):
    high = values.astype(jnp.bfloat16)
    return high, (values - high.astype(jnp.float32)).astype(jnp.bfloat16)


def folded_tables(points, orders):
    tables = []
    for residues, length in (((1, 3), points // 2), ((0,), points // 4), ((2,), points // 4)):
        m = orders[np.isin(orders % 4, residues)]
        angle = 2.0 * np.pi * ((m[:, None] * np.arange(length)[None, :]) % points) / points
        table = np.concatenate([np.cos(angle), -np.sin(angle)]) * points ** -0.5
        table = table.astype(np.float32)
        high = table.astype(jnp.bfloat16)
        low = (table - high.astype(np.float32)).astype(jnp.bfloat16)
        tables.append(np.stack([high, low]))
    return tables


NT = (((1,), (1,)), ((), ()))
TN = (((0,), (0,)), ((), ()))


def dft_kernel(runs, width, pieces, *refs):
    field_refs = refs[:pieces]
    odd_ref, zero_ref, two_ref, out_ref, held = refs[pieces:]
    rows, lats, _ = field_refs[0].shape
    quarter = pieces * LANES // 4
    lines = [ref.reshape(rows * lats, LANES) for ref in field_refs]

    def fetch(lat):
        return [
            jnp.concatenate([line[pl.ds(lat + s, rows, lats), :] for s in range(2)], axis=0)
            for line in lines
        ]

    def transform(table_ref, values):
        high, low = split_bf16(values)
        dot = functools.partial(lax.dot_general, dimension_numbers=NT, preferred_element_type=jnp.float32)
        return dot(table_ref[0], high) + (dot(table_ref[1], high) + dot(table_ref[0], low))

    def put(lat, lane, kind, sums):
        count = sums.shape[0] // 2
        for q in range(2):
            done = 0
            for start in runs[kind]:
                held[q, pl.ds(start * lats + lat, width, lats), :] = (
                    sums[q * count + done:q * count + done + width, lane:lane + LANES]
                )
                done += width

    def step(pair, carry):
        lat = 2 * pair
        values = fetch(lat)
        middle = len(values) // 2
        even = jnp.concatenate([u + v for u, v in zip(values[:middle], values[middle:])], axis=1)
        odd = jnp.concatenate([u - v for u, v in zip(values[:middle], values[middle:])], axis=1)
        parts = (
            transform(odd_ref, odd),
            transform(zero_ref, even[:, :quarter] + even[:, quarter:]),
            transform(two_ref, even[:, :quarter] - even[:, quarter:]),
        )
        for s in range(2):
            for kind, sums in enumerate(parts):
                put(lat + s, s * LANES, kind, sums)
        return carry

    lax.fori_loop(0, lats // 2, step, 0)
    modes = out_ref.shape[0]
    piece = 32

    def emit(index, carry):
        base = pl.multiple_of(index * piece, piece)
        for q in range(2):
            block = held[q, pl.ds(pl.multiple_of(base * lats, piece * lats), piece * lats), :]
            block = block.astype(jnp.bfloat16).reshape(piece, lats, LANES)
            out_ref[pl.ds(base, piece), :, q * LANES:(q + 1) * LANES] = block
        return carry

    lax.fori_loop(0, modes // piece, emit, 0)


def dft(fields, lat_count, orders, modes):
    members, lev_rows, lat_rows, points = fields.shape
    rows = members * lev_rows
    lats = 16
    width = modes // lat_count
    kinds = [[i for i in range(lat_count) if i % 4 in r] for r in ((1, 3), (0,), (2,))]
    runs = [[i * width for i in kind] for kind in kinds]
    tables = [jnp.asarray(t) for t in folded_tables(points, orders)]
    groups = rows // LANES
    pieces = points // LANES
    return pl.pallas_call(
        functools.partial(dft_kernel, runs, width, pieces),
        grid=(lat_rows // lats, groups),
        out_shape=jax.ShapeDtypeStruct((modes, lat_rows, 2 * rows), jnp.bfloat16),
        in_specs=[
            pl.BlockSpec((LANES, lats, LANES), functools.partial(lambda c, l, g: (g, l, c), c))
            for c in range(pieces)
        ]
        + [pl.BlockSpec(t.shape, lambda l, g: (0, 0, 0)) for t in tables],
        out_specs=pl.BlockSpec((modes, lats, 2 * LANES), lambda l, g: (0, l, g)),
        scratch_shapes=[pltpu.VMEM((2, modes * lats, LANES), jnp.float32)],
        compiler_params=pltpu.CompilerParams(vmem_limit_bytes=VMEM_LIMIT),
        cost_estimate=pl.CostEstimate(flops=15_000_000_000, bytes_accessed=65_000_000, transcendentals=0),
    )(*[fields.reshape(rows, lat_rows, points)] * pieces, *tables)


def legendre_kernel(members, lev_rows, band, x_ref, l_ref, out_ref):
    sources, _, slots, lat_rows, lanes = x_ref.shape
    total = l_ref.shape[-1]
    groups = lanes // (2 * LANES)
    for a in range(slots):
        x = x_ref[:, 0, a].reshape(sources * lat_rows, lanes)
        table = l_ref[:, 0, a, :, band * a:]
        table = table.reshape(sources * lat_rows, total - band * a)
        waves = lax.dot_general(table, x, TN, preferred_element_type=jnp.float32)
        for t in range(a, slots):
            block = waves[(t - a) * band:(t - a + 1) * band]
            row = band * (t * (t + 1) // 2 + a)
            for q in range(2):
                parts = [block[:, (2 * g + q) * LANES:(2 * g + q + 1) * LANES] for g in range(groups)]
                total_sum = functools.reduce(jnp.add, parts)
                shift = LANES // 2
                while shift >= lev_rows:
                    total_sum = total_sum + pltpu.roll(total_sum, shift, 1)
                    shift //= 2
                mean = total_sum * (1.0 / members)
                for g in range(groups):
                    out_ref[0, row:row + band, (2 * g + q) * LANES:(2 * g + q + 1) * LANES] = (
                        parts[g] - mean
                    ).astype(jnp.bfloat16)


def covariance_kernel(band, slots, lev_rows, x_ref, out_ref, held):
    sources, _, lanes = x_ref.shape
    pack = LANES // lev_rows
    groups = lanes // LANES
    per_slot = groups * pack
    for t in range(slots):
        start = band * (t * (t + 1) // 2)

        def spread(a, carry):
            row = pl.multiple_of(start + a * band, band)
            for g in range(groups):
                parts = [
                    x_ref[v, pl.ds(row, band), g * LANES:(g + 1) * LANES].astype(jnp.float32)
                    for v in range(sources)
                ]
                for s in range(pack):
                    joined = jnp.concatenate(
                        [p[:, s * lev_rows:(s + 1) * lev_rows] for p in parts], axis=1
                    )
                    place = (a * per_slot + g * pack + s) * band
                    held[pl.ds(pl.multiple_of(place, band), band), :] = joined
            return carry

        lax.fori_loop(0, t + 1, spread, 0)
        depth = (t + 1) * per_slot

        def multiply(n, carry):
            for s in range(4):
                each = n * 4 + s
                values = held[pl.ds(each, depth, band), :].astype(jnp.bfloat16)
                product = lax.dot_general(values, values, TN, preferred_element_type=jnp.float32)
                out_ref[t * band + each] = product.astype(jnp.bfloat16)
            return carry

        lax.fori_loop(0, band // 4, multiply, 0)


def exchange(values, axis):
    return lax.all_to_all(values, axis, split_axis=0, concat_axis=0, tiled=True)


def on_device(lat_count, lev_count, fields, legendre, owner_counts):
    members, lev_rows, lat_rows, points = fields.shape
    modes, totals = legendre.shape[1:]
    owners = owner_counts.shape[0]
    capacity = 2 * modes // owners
    levels = lev_count * lev_rows
    band = lat_count * lev_count
    slots = modes // band
    lanes = 2 * members * lev_rows
    orders = np.arange(modes).reshape(slots, lev_count, lat_count).transpose(2, 1, 0).reshape(-1)

    table = legendre.reshape(lat_rows, slots, lev_count, lat_count, totals).transpose(3, 2, 1, 0, 4)
    table = exchange(table, "lat")
    spectra = dft(fields, lat_count, orders, modes)
    spectra = exchange(spectra.reshape(lat_count, lev_count, slots, lat_rows, lanes), "lat")

    rows = band * slots * (slots + 1) // 2
    anomaly = pl.pallas_call(
        functools.partial(legendre_kernel, members, lev_rows, band),
        grid=(lev_count,),
        out_shape=jax.ShapeDtypeStruct((lev_count, rows, lanes), jnp.bfloat16),
        in_specs=[
            pl.BlockSpec((lat_count, 1, slots, lat_rows, lanes), lambda j: (0, j, 0, 0, 0)),
            pl.BlockSpec((lat_count, 1, slots, lat_rows, totals), lambda j: (0, j, 0, 0, 0)),
        ],
        out_specs=pl.BlockSpec((1, rows, lanes), lambda j: (j, 0, 0)),
        compiler_params=pltpu.CompilerParams(vmem_limit_bytes=VMEM_LIMIT),
        cost_estimate=pl.CostEstimate(flops=4_000_000_000, bytes_accessed=24_000_000, transcendentals=0),
    )(spectra, table)
    anomaly = exchange(anomaly, "lev")

    partial_value = pl.pallas_call(
        functools.partial(covariance_kernel, band, slots, lev_rows),
        out_shape=jax.ShapeDtypeStruct((totals, levels, levels), jnp.bfloat16),
        in_specs=[pl.BlockSpec(memory_space=pltpu.VMEM)],
        out_specs=pl.BlockSpec(memory_space=pltpu.VMEM),
        scratch_shapes=[pltpu.VMEM((slots * 2 * members * band, levels), jnp.float32)],
        compiler_params=pltpu.CompilerParams(vmem_limit_bytes=VMEM_LIMIT),
        cost_estimate=pl.CostEstimate(flops=2_000_000_000, bytes_accessed=16_000_000, transcendentals=0),
    )(anomaly)

    share = totals // lat_count
    partial_value = exchange(partial_value.reshape(lat_count, share, levels, levels), "lat")
    summed = jnp.sum(partial_value.astype(jnp.float32), axis=0)
    summed = summed.reshape(share, lev_count, lev_rows, levels).transpose(1, 0, 2, 3)
    summed = exchange(summed.astype(jnp.bfloat16), "lev")
    full = jnp.sum(summed.astype(jnp.float32), axis=0)
    full = jnp.broadcast_to(full.astype(jnp.bfloat16)[None], (lat_count, share, lev_rows, levels))
    full = exchange(full, "lat").reshape(totals, lev_rows, levels)

    starts = jnp.cumsum(owner_counts) - owner_counts
    owner = lax.axis_index("lat")
    offset = jnp.arange(capacity, dtype=jnp.int32)
    wavenumber = starts[owner] + offset
    live = offset < owner_counts[owner]
    chosen = jnp.take(full, jnp.where(live, wavenumber, 0), axis=0).astype(jnp.float32)
    divisor = ((members - 1) * (2 * wavenumber + 2)).astype(jnp.float32)
    return jnp.where(live[:, None, None], chosen / divisor[:, None, None], jnp.zeros_like(chosen))


def pick(lat_count, lev_count, fields, legendre, owner_counts):
    members, lev_rows, lat_rows, points = fields.shape
    modes = legendre.shape[1]
    fits = (
        lat_rows % 16 == 0
        and members * lev_rows % LANES == 0
        and lev_rows * lev_count == LANES
        and lat_count % 4 == 0
        and modes % (lat_count * lev_count) == 0
    )
    if fits:
        return on_device(lat_count, lev_count, fields, legendre, owner_counts)
    return plain_on_device(fields, legendre, owner_counts)


def solution(mesh):
    return jax.shard_map(
        functools.partial(pick, mesh.shape["lat"], mesh.shape["lev"]),
        mesh=mesh,
        in_specs=(P(None, "lev", "lat", None), P("lat", None, None), P()),
        out_specs=P("lat", "lev", None),
        check_vma=False,
    )
```
